128 devices in a mesh: row: 8 (over y, core), col: 16 (over x, z).
Axes of the slice: x: 4, y: 4, z: 4, core: 2. Of those that a mesh axis runs over, the one named last changes fastest.
Arguments:
- coupling_left: bfloat16 [128, 1024, 2048], P(('row', 'col')), may hold values from -0.75 to 0.75
- inner_factor: bfloat16 [128, 2048, 2048], P(('row', 'col')), as said below
- coupling_right: bfloat16 [128, 2048, 1024], P(('row', 'col')), may hold values from -0.75 to 0.75
- iface_rows: int32 [128, 1024], replicated, may hold values from 0 to 16383, as said below
- interface_diag: float32 [16384], P('row'), may hold values from 2 to 4
- row_scales: float32 [2, 16384], P(None, 'row'), may hold values from 0.5 to 2
- col_scales: float32 [2, 16384], P(None, 'col'), may hold values from 0.5 to 2
Outputs:
- transformed: float32 [16384, 16384], P('row', 'col')
The draws below stay inside these ranges and needn't reach their ends.
Inputs may be any that keep to these rules, and one draw needn't show every extreme that they name: `iface_rows`: each subdomain's list is 8 runs of 128 consecutive rows, each run starting at a multiple of 128, in any order; every tile of 2048 rows holds exactly one run of every subdomain, and no tile of 1024 rows holds two runs of one subdomain. `inner_factor`: lower triangular; its diagonal lies between 0.7 and 1.3.
All inputs are finite; a program needn't handle non-finite values.
Results may differ from the reference program's by a relative error of at most 0.0003.
The reference program's roundings to bfloat16 on the way (of `left_part` and `right_part`) count: a program that leaves them out, or rounds other values in their place, can miss the bound.
Values sent between devices are 32-bit elements; how exact they have to be, the bound alone decides.
A program may use at most 128 MiB of HBM per device.

```python
import math
import jax
import jax.numpy as jnp
from jax import lax

TILE_ROWS = 2048
IROWS = 1024
INNER = 2048
BROWS = 128
IFACE = 16384
TILE_COLS = 1024
BLK = 8
SUBS = 128


def draw_inner_factor(key, part):
    first, second = jax.random.split(jax.random.fold_in(key, 11))
    spread = jax.random.normal(first, (SUBS, INNER, INNER), jnp.float32) * (0.5 / INNER ** 0.5)
    diagonal = jax.random.uniform(second, (SUBS, INNER), jnp.float32, 0.7, 1.3)
    lower = jnp.tril(spread, -1)
    eye_mask = jnp.eye(INNER, dtype=jnp.float32)
    return (lower + eye_mask[None] * diagonal[:, :, None]).astype(jnp.bfloat16)


def draw_iface_rows(key, part):
    rows_count = IFACE // TILE_ROWS
    cols_count = IFACE // TILE_COLS
    per_tile = cols_count // rows_count
    slot_count = BLK // rows_count
    col_blocks = TILE_COLS // BROWS
    first, second, third = jax.random.split(jax.random.fold_in(key, 23), 3)
    raw_score = jax.random.randint(first, (SUBS, rows_count, per_tile), 0, 4)
    offsets = jnp.arange(per_tile, dtype=jnp.int32)
    scores = raw_score * (1 + offsets) * per_tile + offsets
    picked_scores, picked = lax.top_k(scores, slot_count)
    tile_ids = jnp.arange(rows_count, dtype=jnp.int32)[None, :, None] * per_tile + picked.astype(jnp.int32)
    inside = jax.random.randint(second, (SUBS, rows_count, slot_count), 0, col_blocks)
    block_ids = (tile_ids * col_blocks + inside).reshape(SUBS, BLK)
    orders = jax.vmap(lambda sub_key: jax.random.permutation(sub_key, BLK))(jax.random.split(third, SUBS))
    block_ids = jnp.take_along_axis(block_ids, orders.astype(jnp.int32), axis=1)
    rows_all = block_ids[:, :, None] * BROWS + jnp.arange(BROWS, dtype=jnp.int32)[None, None, :]
    return rows_all.reshape(SUBS, IROWS).astype(jnp.int32)


def levels(stream_key, extent, cuts, low, high):
    def one(dim, shards_of):
        steps = jax.random.uniform(jax.random.fold_in(jax.random.fold_in(stream_key, 6), dim), (shards_of,), jnp.float32, low / len(cuts), high / len(cuts))
        return jnp.repeat(jnp.exp(steps), extent[dim] // shards_of).reshape((-1,) + (1,) * (len(extent) - dim - 1))

    factor_of = one(*cuts[0])
    for cut in cuts[1:]:
        factor_of = factor_of * one(*cut)
    return factor_of


def bell_draw(own_key, extent, scale, limit, pieces=(), held_as=jnp.bfloat16):
    values = jax.random.normal(own_key, extent, jnp.float32) * scale
    if len(pieces) > 0:
        values = levels(own_key, extent, pieces, -0.22, 0.18) * values
    return jnp.clip(values, min=-limit, max=limit).astype(held_as)


def setup_inputs(seed: int = 0) -> dict:
    keys = jax.random.split(jax.random.key(seed), 8)
    return {
        "coupling_left": bell_draw(keys[0], (SUBS, IROWS, INNER), (max(1, INNER // 32)) ** -0.5, 0.75, ((0, 128),)),
        "inner_factor": draw_inner_factor(jax.random.fold_in(keys[7], 71), 0),
        "coupling_right": bell_draw(keys[2], (SUBS, INNER, IROWS), (max(1, INNER // 32)) ** -0.5, 0.75, ((0, 128),)),
        "iface_rows": draw_iface_rows(jax.random.fold_in(keys[7], 71), 0),
        "interface_diag": jnp.clip(2.0 + 2.0 * jax.random.uniform(keys[4], (IFACE,), jnp.float32) ** levels(keys[4], (IFACE,), ((0, 8),), -0.2, 0.2), 2.0, 4.0),
        "row_scales": jnp.clip(jnp.exp(math.log(2.0) - 1.3862944 * jax.random.uniform(keys[5], (2, IFACE), jnp.float32) ** levels(keys[5], (2, IFACE), ((1, 8),), -0.2, 0.2)), 0.5, 2.0),
        "col_scales": jnp.clip(jnp.exp(math.log(2.0) - 1.3862944 * jax.random.uniform(keys[6], (2, IFACE), jnp.float32) ** levels(keys[6], (2, IFACE), ((1, 16),), -0.2, 0.2)), 0.5, 2.0),
    }


half_root = 0.5 ** 0.5


def mix_rows(matrix, scales, half_span):
    total = matrix.shape[0]
    shaped = matrix.reshape(total // (2 * half_span), 2, half_span, matrix.shape[1])
    scaled = scales.reshape(total // (2 * half_span), 2, half_span, 1)
    upper = shaped[:, 0]
    lower = shaped[:, 1]
    mixed = jnp.stack([(upper + lower) * scaled[:, 0], (upper - lower) * scaled[:, 1]], axis=1)
    return (mixed * half_root).reshape(total, matrix.shape[1])


def mix_cols(matrix, scales, half_span):
    total = matrix.shape[1]
    shaped = matrix.reshape(matrix.shape[0], total // (2 * half_span), 2, half_span)
    scaled = scales.reshape(1, total // (2 * half_span), 2, half_span)
    upper = shaped[:, :, 0]
    lower = shaped[:, :, 1]
    mixed = jnp.stack([(upper + lower) * scaled[:, :, 0], (upper - lower) * scaled[:, :, 1]], axis=2)
    return (mixed * half_root).reshape(matrix.shape[0], total)


def reference(coupling_left, inner_factor, coupling_right, iface_rows, interface_diag, row_scales, col_scales):
    highest = lax.Precision.HIGHEST
    matrix = jnp.diag(interface_diag.astype(jnp.float32))

    def add_one(which, matrix):
        factor = inner_factor[which].astype(jnp.float32)
        left_part = jnp.dot(coupling_left[which].astype(jnp.float32), factor.T, precision=highest).astype(jnp.bfloat16)
        right_part = jnp.dot(factor, coupling_right[which].astype(jnp.float32), precision=highest).astype(jnp.bfloat16)
        contribution = jnp.dot(left_part.astype(jnp.float32), right_part.astype(jnp.float32), precision=highest)
        places = iface_rows[which].astype(jnp.int32)
        return matrix.at[places[:, None], places[None, :]].add(-contribution)

    matrix = lax.fori_loop(0, SUBS, add_one, matrix)
    matrix = mix_rows(matrix, row_scales[0], IFACE // 4)
    matrix = mix_rows(matrix, row_scales[1], IFACE // 2)
    matrix = mix_cols(matrix, col_scales[0], IFACE // 4)
    matrix = mix_cols(matrix, col_scales[1], IFACE // 2)
    return matrix
```

```python
import functools

import jax
import jax.numpy as jnp
from jax import lax
from jax.experimental import pallas as pl
from jax.experimental.pallas import tpu as pltpu
from jax.sharding import PartitionSpec as P

MESH = pl.DeviceIdType.MESH
F32 = jnp.float32
BF16 = jnp.bfloat16

RUN = 128
INNER = 2048
CHUNK = 256
CHUNKS = INNER // CHUNK
PIECE = 32
PITCH = 40
SRC = 128
STRIPS = 32
TILE = 512
TILE_PITCH = 520
PCHUNK = 4
PSTEPS = 16 // PCHUNK


def position():
    row = lax.axis_index("row")
    col = lax.axis_index("col")
    return col // 4, row // 2, col % 4, row % 2


def device(x, y, z, core):
    return (y * 2 + core, x * 4 + z)


def kernel(
    left_hbm, factor_hbm, right_hbm, iface_hbm, diag_hbm, rows_hbm, cols_hbm,
    out_hbm,
    right_0, right_1, right_2, right_3, right_4, right_5, right_6, right_7, right_p, factor_v, left_v, mixed_v, lpart_v, send1, recv1, tiles, recv2, stage,
    iface_v, rows_v, diag_v, cols_v, cols8, iface_s, rows_s, diag_s,
    in_sem, small_sem, scale_send, scale_recv, send_sem1, zero_sem, recv_sem1, send_sem2, recv_sem2,
    out_sem,
):
    x, y, z, core = position()
    zp, zb = z // 2, z % 2
    me = (y * 2 + core) * 16 + x * 4 + z
    strip = (x * 4 + y) * 2 + zb

    barrier = pltpu.get_barrier_semaphore()

    def greet(o, carry):
        pl.semaphore_signal(
            barrier, inc=1, device_id=((y * 2 + core + o // 16) % 8, (x * 4 + z + o % 16) % 16),
            device_id_type=MESH,
        )
        return carry

    own_rows = pltpu.make_async_copy(
        iface_hbm.at[pl.ds(pl.multiple_of(me // 8 * 8, 8), 8), :], iface_s, small_sem.at[0]
    )
    own_rows.start()
    right_v = [right_0, right_1, right_2, right_3, right_4, right_5, right_6, right_7]
    factor_in = []
    for c in range(CHUNKS):
        rows = pl.ds(c * CHUNK, CHUNK)
        wide = pl.ds(0, (c + 1) * CHUNK)
        for k in range(8):
            pltpu.make_async_copy(
                right_hbm.at[0, rows, pl.ds(k * RUN, RUN)], right_v[c].at[k], in_sem.at[c]
            ).start()
        factor_in.append(
            pltpu.make_async_copy(
                factor_hbm.at[0, rows, wide], factor_v.at[rows, wide], in_sem.at[CHUNKS + c]
            )
        )
        factor_in[c].start()
    left_in = pltpu.make_async_copy(left_hbm, left_v, in_sem.at[2 * CHUNKS])
    left_in.start()
    iface_in = pltpu.make_async_copy(iface_hbm, iface_v, small_sem.at[1])
    iface_in.start()
    rows_in = pltpu.make_async_copy(rows_hbm, rows_v.at[y], small_sem.at[2])
    rows_in.start()
    diag_in = pltpu.make_async_copy(diag_hbm, diag_v.at[y], small_sem.at[3])
    diag_in.start()
    cols_in = pltpu.make_async_copy(cols_hbm, cols_v.at[x * 2 + zb], small_sem.at[4])
    cols_in.start()
    lax.fori_loop(1, SRC, greet, 0)
    own_rows.wait()

    run_tile = [lax.div(iface_s[me % 8, RUN * k], 16 * RUN) for k in range(8)]

    def run_in(j):
        found = jnp.int32(0)
        for k in range(1, 8):
            found += k * (run_tile[k] == j).astype(jnp.int32)
        return found & 7

    run_of = [run_in(j) for j in range(8)]

    for c in range(CHUNKS):
        rows = pl.ds(c * CHUNK, CHUNK)
        deep = (c + 1) * CHUNK
        pltpu.make_async_copy(right_v[c], right_v[c], in_sem.at[c]).wait()
        for m in range(8):
            right_p[rows, m * RUN : (m + 1) * RUN] = right_v[c][run_of[m]]
        factor_in[c].wait()
        mixed_v[rows, :] = jnp.dot(
            factor_v[rows, :deep], right_p[:deep, :], preferred_element_type=F32
        ).astype(BF16)
    left_in.wait()

    def send_group(g, carry):
        half, to_core = g // 2, g % 2
        runs = [run_in((half * 2 + y1) * 2 + to_core) for y1 in range(2)]
        for c in range(CHUNKS):
            rows = pl.ds(c * CHUNK, CHUNK)
            deep = (c + 1) * CHUNK
            taken = jnp.concatenate([left_v[run, :, :deep] for run in runs], axis=0)
            lpart_v[:, c * CHUNK : (c + 1) * CHUNK] = lax.dot_general(
                taken, factor_v[rows, :deep], (((1,), (1,)), ((), ())), preferred_element_type=F32
            ).astype(BF16)
        for pair in range(4):
            block = jnp.dot(
                lpart_v[...], mixed_v[:, pair * 2 * RUN : (pair + 1) * 2 * RUN],
                preferred_element_type=F32,
            )
            for half_pair in range(2):
                for y1 in range(2):
                    for i in range(4):
                        for t8 in range(4):
                            row = y1 * RUN + 32 * i + 8 * t8
                            base = (half_pair * 32 + 8 * t8) * PITCH + y1 * 16 + pair * 4 + i
                            send1[pl.ds(g * (64 * PITCH) + base, 8, stride=PITCH), :] = block[
                                row : row + 8, half_pair * RUN : (half_pair + 1) * RUN
                            ]

        @pl.when(g == 0)
        def _():
            pl.semaphore_wait(barrier, SRC - 1)

        def piece(px, py, pz):
            index = g * 64 + (pz // 2) * 32 + (px * 4 + py) * 2 + pz % 2
            return (
                send1.at[pl.ds(pl.multiple_of(index * PITCH, 8), PIECE), :],
                recv1.at[pl.ds(pl.multiple_of((half * SRC + me) * PITCH, 8), PIECE), :],
            )

        @pl.when(to_core == core)
        def _():
            src, dst = piece(x, y, z)
            pltpu.make_async_copy(src, dst, recv_sem1.at[half]).start()

        @pl.when(to_core != core)
        def _():
            src, dst = piece(x, y, z)
            pltpu.make_async_remote_copy(
                src, dst, zero_sem.at[half], recv_sem1.at[half],
                device_id=device(x, y, z, to_core), device_id_type=MESH,
            ).start()

        def one(o, inner):
            o = (o * 27) % 64
            px, py, pz = (x + o % 4) % 4, (y + o // 4 % 4) % 4, (z + o // 16) % 4
            src, dst = piece(px, py, pz)
            pltpu.make_async_remote_copy(
                src, dst, send_sem1.at[g], recv_sem1.at[half],
                device_id=device(px, py, pz, to_core), device_id_type=MESH,
            ).start()
            return inner

        lax.fori_loop(1, 64, one, 0)
        return carry

    lax.fori_loop(0, 4, send_group, 0)

    rows_in.wait()
    diag_in.wait()
    cols_in.wait()
    for d in range(1, 4):
        to = device(x, (y + d) % 4, z, core)
        pltpu.make_async_remote_copy(
            rows_v.at[y], rows_v.at[y], scale_send.at[d], scale_recv.at[d], device_id=to,
            device_id_type=MESH,
        ).start()
        pltpu.make_async_remote_copy(
            diag_v.at[y], diag_v.at[y], scale_send.at[3 + d], scale_recv.at[3 + d], device_id=to,
            device_id_type=MESH,
        ).start()
    for d in range(1, 8):
        pltpu.make_async_remote_copy(
            cols_v.at[x * 2 + zb], cols_v.at[x * 2 + zb], scale_send.at[6 + d],
            scale_recv.at[6 + d],
            device_id=device((x + d // 2) % 4, y, zp * 2 + (zb + d % 2) % 2, core),
            device_id_type=MESH,
        ).start()

    iface_in.wait()
    run_ids = []
    for k in range(8):
        run_ids.append(lax.div(iface_v[:, k * RUN : (k + 1) * RUN].T[0:1, :], RUN))

    def placed(j):
        total = jnp.zeros((1, SRC), jnp.int32)
        for k in range(8):
            total += jnp.where(run_ids[k] // 16 == j, run_ids[k] % 16, 0)
        return total

    col_place = [placed(2 * j + zp) for j in range(4)]
    row_place = [placed(2 * j + core) for j in range(4)]
    spots = lax.broadcasted_iota(jnp.int32, (256, SRC), 0)

    for half in range(2):
        got = recv1.at[pl.ds(0, SRC * PIECE), :]
        pltpu.make_async_copy(got, got, recv_sem1.at[half]).wait()
        for y1 in range(2):
            for xx in range(4):
                first = half * SRC * PITCH + y1 * 16 + xx * 4
                data = jnp.concatenate(
                    [recv1[pl.ds(first + i, SRC, stride=PITCH), :] for i in range(4)], axis=1
                )
                high = data.astype(BF16)
                low = (data - high.astype(F32)).astype(BF16)
                spot = row_place[half * 2 + y1] * 16 + col_place[xx]
                hot = jnp.where(spots == spot, -1.0, 0.0).astype(BF16)
                tile = jnp.dot(
                    jnp.concatenate([hot, hot], axis=1), jnp.concatenate([high, low], axis=0),
                    preferred_element_type=F32,
                )
                for zz in range(2):
                    base = (((half * 2 + y1) * 4 + xx) * 2 + zz) * TILE
                    for p in range(16):
                        for i in range(4):
                            tiles[base + p * 32 + i * 8 : base + p * 32 + i * 8 + 8, :] = tile[
                                p * 16 + zz * 8 : p * 16 + zz * 8 + 8, i * 128 : (i + 1) * 128
                            ]

    for d in range(1, 4):
        rows_v_any, diag_v_any = rows_v.at[y], diag_v.at[y]
        pltpu.make_async_remote_copy(
            rows_v_any, rows_v_any, scale_send.at[d], scale_recv.at[d],
            device_id=device(x, y, z, core), device_id_type=MESH,
        ).wait()
        pltpu.make_async_remote_copy(
            diag_v_any, diag_v_any, scale_send.at[3 + d], scale_recv.at[3 + d],
            device_id=device(x, y, z, core), device_id_type=MESH,
        ).wait()
    for d in range(1, 8):
        cols_any = cols_v.at[x * 2 + zb]
        pltpu.make_async_remote_copy(
            cols_any, cols_any, scale_send.at[6 + d], scale_recv.at[6 + d],
            device_id=device(x, y, z, core), device_id_type=MESH,
        ).wait()
    rows_to = pltpu.make_async_copy(rows_v, rows_s, small_sem.at[2])
    diag_to = pltpu.make_async_copy(diag_v, diag_s, small_sem.at[3])
    rows_to.start()
    diag_to.start()
    for xz in range(8):
        for level in range(2):
            for q in range(8):
                cols8[xz, level, q : q + 1, :] = cols_v[
                    xz, level : level + 1, q * 128 : (q + 1) * 128
                ] * (1.0 if level == 0 else 0.25)
    rows_to.wait()
    diag_to.wait()

    sub8 = lax.broadcasted_iota(jnp.int32, (8, 128), 0)
    lane8 = lax.broadcasted_iota(jnp.int32, (8, 128), 1)

    for step in range(PSTEPS):

        def mix(pp, carry):
            p = step * PCHUNK + pp
            for zz in range(2):
                first = [cols8[xx * 2 + zz, 0] for xx in range(4)]
                second = [cols8[xx * 2 + zz, 1] for xx in range(4)]
                for i in range(4):
                    spot = p * RUN + 32 * i + strip
                    on = (sub8 + 8 * zz == p) & (lane8 == 32 * i + strip) & (core == zp)

                    def at(yy, xx):
                        start = ((yy * 4 + xx) * 2 + zz) * TILE + p * 32 + i * 8
                        return pl.ds(pl.multiple_of(start, 8), 8)

                    s0 = [rows_s[yy, 0, spot] for yy in range(4)]
                    s1 = [rows_s[yy, 1, spot] for yy in range(4)]
                    held = [[None] * 4 for _ in range(4)]
                    for xx in range(4):
                        a = [tiles[at(yy, xx), :] for yy in range(4)]
                        a[xx] = a[xx] + jnp.where(on, diag_s[xx, 0, spot], 0.0)
                        b0, b1 = (a[0] + a[1]) * s0[0], (a[0] - a[1]) * s0[1]
                        b2, b3 = (a[2] + a[3]) * s0[2], (a[2] - a[3]) * s0[3]
                        held[0][xx] = (b0 + b2) * s1[0]
                        held[2][xx] = (b0 - b2) * s1[2]
                        held[1][xx] = (b1 + b3) * s1[1]
                        held[3][xx] = (b1 - b3) * s1[3]
                    for yy in range(4):
                        a = held[yy]
                        b0, b1 = (a[0] + a[1]) * first[0], (a[0] - a[1]) * first[1]
                        b2, b3 = (a[2] + a[3]) * first[2], (a[2] - a[3]) * first[3]
                        tiles[at(yy, 0), :] = (b0 + b2) * second[0]
                        tiles[at(yy, 2), :] = (b0 - b2) * second[2]
                        tiles[at(yy, 1), :] = (b1 + b3) * second[1]
                        tiles[at(yy, 3), :] = (b1 - b3) * second[3]
            return carry

        lax.fori_loop(0, PCHUNK, mix, 0)

        def back(px, py, pzb):
            index = (py * 4 + px) * 2 + pzb
            return (
                tiles.at[pl.ds(pl.multiple_of(index * TILE + step * PCHUNK * 32, 8), PCHUNK * 32), :],
                recv2.at[
                    pl.ds(pl.multiple_of(strip * TILE_PITCH + step * PCHUNK * 32, 8), PCHUNK * 32), :
                ],
            )

        src, dst = back(x, y, zb)
        pltpu.make_async_copy(src, dst, recv_sem2.at[step]).start()

        def one_back(o, carry):
            o = (o * 11) % 32
            px, py, pzb = (x + o % 4) % 4, (y + o // 4 % 4) % 4, (zb + o // 16) % 2
            src, dst = back(px, py, pzb)
            pltpu.make_async_remote_copy(
                src, dst, send_sem2.at[step], recv_sem2.at[step],
                device_id=device(px, py, zp * 2 + pzb, core), device_id_type=MESH,
            ).start()
            return carry

        lax.fori_loop(1, STRIPS, one_back, 0)

    def put(p, slot):
        return pltpu.make_async_copy(
            stage.at[slot], out_hbm.at[pl.ds(pl.multiple_of(p * RUN, RUN), RUN), :], out_sem.at[slot]
        )

    for step in range(PSTEPS):
        got = recv2.at[pl.ds(0, STRIPS * PCHUNK * 32), :]
        pltpu.make_async_copy(got, got, recv_sem2.at[step]).wait()
        for pp in range(PCHUNK):
            p = step * PCHUNK + pp
            slot = p % 4
            if p >= 4:
                put(p - 4, slot).wait()

            def merge(i, carry):
                for a in range(4):
                    for q in range(8):
                        stage[
                            slot, pl.ds(pl.multiple_of(32 * i + 8 * a, 8), 8), q * 128 : (q + 1) * 128
                        ] = recv2[
                            pl.ds(8 * a * TILE_PITCH + p * 32 + i * 8 + q, 8, stride=TILE_PITCH), :
                        ]
                return carry

            lax.fori_loop(0, 4, merge, 0)
            put(p, slot).start()
    for p in range(12, 16):
        put(p, p % 4).wait()

    for g in range(4):
        sent = send1.at[pl.ds(0, 63 * PIECE), :]
        pltpu.make_async_copy(sent, sent, send_sem1.at[g]).wait()
    for half in range(2):
        sent = send1.at[pl.ds(0, PIECE), :]
        pltpu.make_async_copy(sent, sent, zero_sem.at[half]).wait()
    for step in range(PSTEPS):
        sent = tiles.at[pl.ds(0, (STRIPS - 1) * PCHUNK * 32), :]
        pltpu.make_async_copy(sent, sent, send_sem2.at[step]).wait()


def body(
    coupling_left, inner_factor, coupling_right, iface_rows, interface_diag, row_scales, col_scales
):
    any_space = pl.BlockSpec(memory_space=pl.ANY)
    return pl.pallas_call(
        kernel,
        out_shape=jax.ShapeDtypeStruct((2048, 1024), F32),
        in_specs=[any_space] * 7,
        out_specs=any_space,
        scratch_shapes=[
            *[pltpu.VMEM((8, CHUNK, RUN), BF16)] * CHUNKS,
            pltpu.VMEM((INNER, 1024), BF16),
            pltpu.VMEM((INNER, INNER), BF16),
            pltpu.VMEM((8, RUN, INNER), BF16),
            pltpu.VMEM((INNER, 1024), BF16),
            pltpu.VMEM((2 * RUN, INNER), BF16),
            pltpu.VMEM((4 * 64 * PITCH, 128), F32),
            pltpu.VMEM((2 * SRC * PITCH, 128), F32),
            pltpu.VMEM((STRIPS * TILE, 128), F32),
            pltpu.VMEM((STRIPS * TILE_PITCH, 128), F32),
            pltpu.VMEM((4, RUN, 1024), F32),
            pltpu.VMEM((SRC, 1024), jnp.int32),
            pltpu.VMEM((4, 2, 2048), F32),
            pltpu.VMEM((4, 1, 2048), F32),
            pltpu.VMEM((8, 2, 1024), F32),
            pltpu.VMEM((8, 2, 8, 128), F32),
            pltpu.SMEM((8, 1024), jnp.int32),
            pltpu.SMEM((4, 2, 2048), F32),
            pltpu.SMEM((4, 1, 2048), F32),
            pltpu.SemaphoreType.DMA((2 * CHUNKS + 1,)),
            pltpu.SemaphoreType.DMA((5,)),
            pltpu.SemaphoreType.DMA((14,)),
            pltpu.SemaphoreType.DMA((14,)),
            pltpu.SemaphoreType.DMA((4,)),
            pltpu.SemaphoreType.DMA((2,)),
            pltpu.SemaphoreType.DMA((2,)),
            pltpu.SemaphoreType.DMA((PSTEPS,)),
            pltpu.SemaphoreType.DMA((PSTEPS,)),
            pltpu.SemaphoreType.DMA((4,)),
        ],
        compiler_params=pltpu.CompilerParams(
            collective_id=0, has_side_effects=True, vmem_limit_bytes=63 * 2**20
        ),
    )(
        coupling_left.reshape(8, RUN, INNER), inner_factor, coupling_right, iface_rows, interface_diag[None, :],
        row_scales, col_scales,
    )


def solution(mesh):
    in_specs = (
        P(("row", "col"), None, None),
        P(("row", "col"), None, None),
        P(("row", "col"), None, None),
        P(),
        P("row"),
        P(None, "row"),
        P(None, "col"),
    )
    out_specs = P("row", "col")
    return jax.shard_map(body, mesh=mesh, in_specs=in_specs, out_specs=out_specs, check_vma=False)
```

```python
import functools

import jax
import jax.numpy as jnp
from jax import lax
from jax.experimental import pallas as pl
from jax.experimental.pallas import tpu as pltpu
from jax.sharding import PartitionSpec as P

MESH = pl.DeviceIdType.MESH
F32 = jnp.float32
BF16 = jnp.bfloat16

VLIM = 63 * 2**20
RUN = 128
INNER = 2048
CHUNK = 256
CHUNKS = INNER // CHUNK
PIECE = 32
PITCH = 40
SRC = 128
STRIPS = 32
TILE = 512
TILE_PITCH = 512
SET = TILE // 2
PCHUNK = 8
PSTEPS = 16 // PCHUNK


def position():
    row = lax.axis_index("row")
    col = lax.axis_index("col")
    return col // 4, row // 2, col % 4, row % 2


def device(x, y, z, core):
    return (y * 2 + core, x * 4 + z)


def kernel(
    left_hbm, factor_hbm, right_hbm, iface_hbm, diag_hbm, rows_hbm, cols_hbm,
    recv2,
    right_0, right_1, right_2, right_3, right_4, right_5, right_6, right_7, right_p, factor_v, left_v, mixed_v, lpart_v, send1, recv1, tiles,
    iface_v, rows_v, diag_v, cols_v, cols8, iface_s, rows_s, diag_s,
    in_sem, small_sem, scale_send, scale_recv, send_sem1, zero_sem, recv_sem1, send_sem2, recv_sem2,
):
    x, y, z, core = position()
    zp, zb = z // 2, z % 2
    me = (y * 2 + core) * 16 + x * 4 + z
    strip = (x * 4 + y) * 2 + zb

    barrier = pltpu.get_barrier_semaphore()

    def greet(o, carry):
        pl.semaphore_signal(
            barrier, inc=1, device_id=((y * 2 + core + o // 16) % 8, (x * 4 + z + o % 16) % 16),
            device_id_type=MESH,
        )
        return carry

    own_rows = pltpu.make_async_copy(
        iface_hbm.at[pl.ds(pl.multiple_of(me // 8 * 8, 8), 8), :], iface_s, small_sem.at[0]
    )
    own_rows.start()
    right_v = [right_0, right_1, right_2, right_3, right_4, right_5, right_6, right_7]
    factor_in = []
    for c in range(CHUNKS):
        rows = pl.ds(c * CHUNK, CHUNK)
        wide = pl.ds(0, (c + 1) * CHUNK)
        for k in range(8):
            pltpu.make_async_copy(
                right_hbm.at[0, rows, pl.ds(k * RUN, RUN)], right_v[c].at[k], in_sem.at[c]
            ).start()
        factor_in.append(
            pltpu.make_async_copy(
                factor_hbm.at[0, rows, wide], factor_v.at[rows, wide], in_sem.at[CHUNKS + c]
            )
        )
        factor_in[c].start()
    left_in = pltpu.make_async_copy(left_hbm, left_v, in_sem.at[2 * CHUNKS])
    left_in.start()
    iface_in = pltpu.make_async_copy(iface_hbm, iface_v, small_sem.at[1])
    iface_in.start()
    rows_in = pltpu.make_async_copy(rows_hbm, rows_v.at[y], small_sem.at[2])
    rows_in.start()
    diag_in = pltpu.make_async_copy(diag_hbm, diag_v.at[y], small_sem.at[3])
    diag_in.start()
    cols_in = pltpu.make_async_copy(cols_hbm, cols_v.at[x * 2 + zb], small_sem.at[4])
    cols_in.start()
    lax.fori_loop(1, SRC, greet, 0)
    own_rows.wait()

    run_tile = [lax.div(iface_s[me % 8, RUN * k], 16 * RUN) for k in range(8)]

    def run_in(j):
        found = jnp.int32(0)
        for k in range(1, 8):
            found += k * (run_tile[k] == j).astype(jnp.int32)
        return found & 7

    run_of = [run_in(j) for j in range(8)]

    for c in range(CHUNKS):
        rows = pl.ds(c * CHUNK, CHUNK)
        deep = (c + 1) * CHUNK
        pltpu.make_async_copy(right_v[c], right_v[c], in_sem.at[c]).wait()
        for m in range(8):
            right_p[rows, m * RUN : (m + 1) * RUN] = right_v[c][run_of[m]]
        factor_in[c].wait()
        mixed_v[rows, :] = jnp.dot(
            factor_v[rows, :deep], right_p[:deep, :], preferred_element_type=F32
        ).astype(BF16)
    left_in.wait()

    def send_group(g, carry):
        half, to_core = g // 2, g % 2
        runs = [run_in((half * 2 + y1) * 2 + to_core) for y1 in range(2)]
        for c in range(CHUNKS):
            rows = pl.ds(c * CHUNK, CHUNK)
            deep = (c + 1) * CHUNK
            taken = jnp.concatenate([left_v[run, :, :deep] for run in runs], axis=0)
            lpart_v[:, c * CHUNK : (c + 1) * CHUNK] = lax.dot_general(
                taken, factor_v[rows, :deep], (((1,), (1,)), ((), ())), preferred_element_type=F32
            ).astype(BF16)
        for pair in range(4):
            block = jnp.dot(
                lpart_v[...], mixed_v[:, pair * 2 * RUN : (pair + 1) * 2 * RUN],
                preferred_element_type=F32,
            )
            for half_pair in range(2):
                for y1 in range(2):
                    slot = y1 * 4 + pair
                    for b in range(16):
                        base = ((b // 8) * 4 * 64 + half_pair * 32 + 4 * (b % 8)) * 16 + slot
                        send1[pl.ds((to_core * 2 + half) * (64 * 16) + base, 8, stride=8), :] = block[
                            y1 * RUN + 8 * b : y1 * RUN + 8 * b + 8,
                            half_pair * RUN : (half_pair + 1) * RUN,
                        ]

        @pl.when(g == 0)
        def _():
            pl.semaphore_wait(barrier, SRC - 1)
            rows_in.wait()
            diag_in.wait()
            cols_in.wait()
            for d in range(1, 4):
                to = device(x, (y + d) % 4, z, core)
                pltpu.make_async_remote_copy(
                    rows_v.at[y], rows_v.at[y], scale_send.at[d], scale_recv.at[d], device_id=to,
                    device_id_type=MESH,
                ).start()
                pltpu.make_async_remote_copy(
                    diag_v.at[y], diag_v.at[y], scale_send.at[3 + d], scale_recv.at[3 + d], device_id=to,
                    device_id_type=MESH,
                ).start()
            for d in range(1, 8):
                pltpu.make_async_remote_copy(
                    cols_v.at[x * 2 + zb], cols_v.at[x * 2 + zb], scale_send.at[6 + d],
                    scale_recv.at[6 + d],
                    device_id=device((x + d // 2) % 4, y, zp * 2 + (zb + d % 2) % 2, core),
                    device_id_type=MESH,
                ).start()

        send_pieces(0, to_core, half, send_sem1.at[g], zero_sem.at[half])
        return carry

    def send_pieces(part, to_core, half, sent, sent_zero):
        def piece(px, py, pz):
            index = (part * 4 + to_core * 2 + half) * 64 + (pz // 2) * 32
            index += (px * 4 + py) * 2 + pz % 2
            return (
                send1.at[pl.ds(pl.multiple_of(index * 16, 8), 16), :],
                recv1.at[pl.ds(pl.multiple_of((part * SRC + me) * PITCH + half * 16, 8), 16), :],
            )

        @pl.when(to_core == core)
        def _():
            src, dst = piece(x, y, z)
            pltpu.make_async_copy(src, dst, recv_sem1.at[part]).start()

        @pl.when(to_core != core)
        def _():
            src, dst = piece(x, y, z)
            pltpu.make_async_remote_copy(
                src, dst, sent_zero, recv_sem1.at[part],
                device_id=device(x, y, z, to_core), device_id_type=MESH,
            ).start()

        def one(o, inner):
            o = (o * 27) % 64
            px, py, pz = (x + o % 4) % 4, (y + o // 4 % 4) % 4, (z + o // 16) % 4
            src, dst = piece(px, py, pz)
            pltpu.make_async_remote_copy(
                src, dst, sent, recv_sem1.at[part],
                device_id=device(px, py, pz, to_core), device_id_type=MESH,
            ).start()
            return inner

        lax.fori_loop(1, 64, one, 0)

    lax.fori_loop(0, 4, send_group, 0)

    def send_rest(g, carry):
        send_pieces(1, g % 2, g // 2, send_sem1.at[4 + g], zero_sem.at[2 + g // 2])
        return carry

    lax.fori_loop(0, 4, send_rest, 0)

    iface_in.wait()
    run_ids = []
    for k in range(8):
        run_ids.append(lax.div(iface_v[:, k * RUN : (k + 1) * RUN].T[0:1, :], RUN))

    def placed(j):
        total = jnp.zeros((1, SRC), jnp.int32)
        for k in range(8):
            total += jnp.where(run_ids[k] // 16 == j, run_ids[k] % 16, 0)
        return total

    col_place = [placed(2 * j + zp) for j in range(4)]
    row_place = [placed(2 * j + core) for j in range(4)]
    spots = lax.broadcasted_iota(jnp.int32, (256, SRC), 0)

    def place(part):
        got = recv1.at[pl.ds(0, SRC * PIECE), :]
        pltpu.make_async_copy(got, got, recv_sem1.at[part]).wait()
        for yy in range(4):
            for xx in range(4):
                first = part * SRC * PITCH + (yy // 2) * 16 + (yy % 2) * 4 + xx
                data = jnp.concatenate(
                    [recv1[pl.ds(first + 8 * i, SRC, stride=PITCH), :] for i in range(2)], axis=1
                )
                high = data.astype(BF16)
                low = (data - high.astype(F32)).astype(BF16)
                spot = row_place[yy] * 16 + col_place[xx]
                hot = jnp.where(spots == spot, -1.0, 0.0).astype(BF16)
                tile = jnp.dot(
                    jnp.concatenate([hot, hot], axis=1), jnp.concatenate([high, low], axis=0),
                    preferred_element_type=F32,
                )
                for zz in range(2):
                    base = ((yy * 4 + xx) * 2 + zz) * TILE + part * SET
                    for p in range(16):
                        for i in range(2):
                            tiles[pl.ds(base + p * 16 + i, 8, stride=2), :] = tile[
                                p * 16 + zz * 8 : p * 16 + zz * 8 + 8, i * 128 : (i + 1) * 128
                            ]

    place(0)
    for d in range(1, 4):
        rows_v_any, diag_v_any = rows_v.at[y], diag_v.at[y]
        pltpu.make_async_remote_copy(
            rows_v_any, rows_v_any, scale_send.at[d], scale_recv.at[d],
            device_id=device(x, y, z, core), device_id_type=MESH,
        ).wait()
        pltpu.make_async_remote_copy(
            diag_v_any, diag_v_any, scale_send.at[3 + d], scale_recv.at[3 + d],
            device_id=device(x, y, z, core), device_id_type=MESH,
        ).wait()
    for d in range(1, 8):
        cols_any = cols_v.at[x * 2 + zb]
        pltpu.make_async_remote_copy(
            cols_any, cols_any, scale_send.at[6 + d], scale_recv.at[6 + d],
            device_id=device(x, y, z, core), device_id_type=MESH,
        ).wait()
    rows_to = pltpu.make_async_copy(rows_v, rows_s, small_sem.at[2])
    diag_to = pltpu.make_async_copy(diag_v, diag_s, small_sem.at[3])
    rows_to.start()
    diag_to.start()
    for xz in range(8):
        for level in range(2):
            for q in range(8):
                cols8[xz, level, q // 4, q % 4 * 2 : q % 4 * 2 + 2, :] = jnp.broadcast_to(
                    cols_v[xz, level : level + 1, q * 128 : (q + 1) * 128]
                    * (1.0 if level == 0 else 0.25),
                    (2, 128),
                )
    rows_to.wait()
    diag_to.wait()

    sub8 = lax.broadcasted_iota(jnp.int32, (8, 128), 0)
    lane8 = lax.broadcasted_iota(jnp.int32, (8, 128), 1)
    odd = sub8 % 2 == 1

    def mix_and_send(part, step):

        def mix(pp, carry):
            p = step * PCHUNK + pp
            within = 64 * part + 2 * strip
            spot = p * RUN + within
            s0 = [jnp.where(odd, rows_s[yy, 0, spot + 1], rows_s[yy, 0, spot]) for yy in range(4)]
            s1 = [jnp.where(odd, rows_s[yy, 1, spot + 1], rows_s[yy, 1, spot]) for yy in range(4)]
            diags = [
                jnp.where(odd, diag_s[yy, 0, spot + 1], diag_s[yy, 0, spot]) for yy in range(4)
            ]
            for zz in range(2):
                for h in range(2):
                    first = [cols8[xx * 2 + zz, 0, h] for xx in range(4)]
                    second = [cols8[xx * 2 + zz, 1, h] for xx in range(4)]
                    on = (sub8 // 2 + 8 * zz + 4 * h == p) & (lane8 == within + sub8 % 2)
                    on = on & (core == zp)

                    def at(yy, xx):
                        start = ((yy * 4 + xx) * 2 + zz) * TILE + part * SET + p * 16 + h * 8
                        return pl.ds(pl.multiple_of(start, 8), 8)

                    held = [[None] * 4 for _ in range(4)]
                    for xx in range(4):
                        a = [tiles[at(yy, xx), :] for yy in range(4)]
                        a[xx] = a[xx] + jnp.where(on, diags[xx], 0.0)
                        b0, b1 = (a[0] + a[1]) * s0[0], (a[0] - a[1]) * s0[1]
                        b2, b3 = (a[2] + a[3]) * s0[2], (a[2] - a[3]) * s0[3]
                        held[0][xx] = (b0 + b2) * s1[0]
                        held[2][xx] = (b0 - b2) * s1[2]
                        held[1][xx] = (b1 + b3) * s1[1]
                        held[3][xx] = (b1 - b3) * s1[3]
                    for yy in range(4):
                        a = held[yy]
                        b0, b1 = (a[0] + a[1]) * first[0], (a[0] - a[1]) * first[1]
                        b2, b3 = (a[2] + a[3]) * first[2], (a[2] - a[3]) * first[3]
                        tiles[at(yy, 0), :] = (b0 + b2) * second[0]
                        tiles[at(yy, 2), :] = (b0 - b2) * second[2]
                        tiles[at(yy, 1), :] = (b1 + b3) * second[1]
                        tiles[at(yy, 3), :] = (b1 - b3) * second[3]
            return carry

        lax.fori_loop(0, PCHUNK, mix, 0)

        chunk = part * SET + step * PCHUNK * 16

        def back(px, py, pzb):
            index = (py * 4 + px) * 2 + pzb
            return (
                tiles.at[pl.ds(pl.multiple_of(index * TILE + chunk, 8), PCHUNK * 16), :],
                recv2.at[pl.ds(pl.multiple_of(strip * TILE_PITCH + chunk, 8), PCHUNK * 16), :],
            )

        src, dst = back(x, y, zb)
        order = part * PSTEPS + step
        pltpu.make_async_copy(src, dst, recv_sem2.at[order]).start()

        def one_back(o, carry):
            o = (o * 11) % 32
            px, py, pzb = (x + o % 4) % 4, (y + o // 4 % 4) % 4, (zb + o // 16) % 2
            src, dst = back(px, py, pzb)
            pltpu.make_async_remote_copy(
                src, dst, send_sem2.at[order], recv_sem2.at[order],
                device_id=device(px, py, zp * 2 + pzb, core), device_id_type=MESH,
            ).start()
            return carry

        lax.fori_loop(1, STRIPS, one_back, 0)

    for step in range(PSTEPS):
        mix_and_send(0, step)
    place(1)
    for step in range(PSTEPS):
        mix_and_send(1, step)

    for order in range(2 * PSTEPS):
        got = recv2.at[pl.ds(0, STRIPS * PCHUNK * 16), :]
        pltpu.make_async_copy(got, got, recv_sem2.at[order]).wait()

    for g in range(8):
        sent = send1.at[pl.ds(0, 63 * 16), :]
        pltpu.make_async_copy(sent, sent, send_sem1.at[g]).wait()
    for half in range(2):
        sent = send1.at[pl.ds(0, 16), :]
        pltpu.make_async_copy(sent, sent, zero_sem.at[half]).wait()
        sent = send1.at[pl.ds(0, 16), :]
        pltpu.make_async_copy(sent, sent, zero_sem.at[2 + half]).wait()
    for order in range(2 * PSTEPS):
        sent = tiles.at[pl.ds(0, (STRIPS - 1) * PCHUNK * 16), :]
        pltpu.make_async_copy(sent, sent, send_sem2.at[order]).wait()


def merge(strips, out, got, held, in_sem, out_sem):
    sub8 = lax.broadcasted_iota(jnp.int32, (8, 128), 0)
    upper = sub8 < 4
    even = sub8 // 2 % 2 == 0

    def fetch(p, part):
        return pltpu.make_async_copy(
            strips.at[:, pl.ds(pl.multiple_of(part * SET + p * 16, 8), 16), :],
            got.at[p, part], in_sem.at[p],
        )

    def put(p):
        return pltpu.make_async_copy(
            held.at[p], out.at[pl.ds(pl.multiple_of(p * RUN, RUN), RUN), :], out_sem.at[p]
        )

    def start(p, carry):
        for part in range(2):
            fetch(p, part).start()
        return carry

    lax.fori_loop(0, 16, start, 0)

    def swap(a, b, mask, shift):
        return (
            jnp.where(mask, a, pltpu.roll(b, shift, 0)),
            jnp.where(mask, pltpu.roll(a, 8 - shift, 0), b),
        )

    def one(p, carry):
        pltpu.make_async_copy(got.at[p], got.at[p], in_sem.at[p]).wait()
        for part in range(2):
            for a in range(8):
                for h in range(2):
                    v = [got[p, part, 4 * a + k, 8 * h : 8 * h + 8, :] for k in range(4)]
                    v[0], v[2] = swap(v[0], v[2], upper, 4)
                    v[1], v[3] = swap(v[1], v[3], upper, 4)
                    v[0], v[1] = swap(v[0], v[1], even, 2)
                    v[2], v[3] = swap(v[2], v[3], even, 2)
                    for k in range(4):
                        q = 4 * h + k
                        held[
                            p, 64 * part + 8 * a : 64 * part + 8 * a + 8, q * 128 : (q + 1) * 128
                        ] = v[k]
        put(p).start()
        return carry

    lax.fori_loop(0, 16, one, 0)

    def finish(p, carry):
        put(p).wait()
        return carry

    lax.fori_loop(0, 16, finish, 0)


def body(
    coupling_left, inner_factor, coupling_right, iface_rows, interface_diag, row_scales, col_scales
):
    any_space = pl.BlockSpec(memory_space=pl.ANY)
    strips = pl.pallas_call(
        kernel,
        out_shape=jax.ShapeDtypeStruct((STRIPS * TILE_PITCH, 128), F32),
        in_specs=[any_space] * 7,
        out_specs=any_space,
        scratch_shapes=[
            *[pltpu.VMEM((8, CHUNK, RUN), BF16)] * CHUNKS,
            pltpu.VMEM((INNER, 1024), BF16),
            pltpu.VMEM((INNER, INNER), BF16),
            pltpu.VMEM((8, RUN, INNER), BF16),
            pltpu.VMEM((INNER, 1024), BF16),
            pltpu.VMEM((2 * RUN, INNER), BF16),
            pltpu.VMEM((2 * 4 * 64 * 16, 128), F32),
            pltpu.VMEM((2 * SRC * PITCH, 128), F32),
            pltpu.VMEM((STRIPS * TILE, 128), F32),
            pltpu.VMEM((SRC, 1024), jnp.int32),
            pltpu.VMEM((4, 2, 2048), F32),
            pltpu.VMEM((4, 1, 2048), F32),
            pltpu.VMEM((8, 2, 1024), F32),
            pltpu.VMEM((8, 2, 2, 8, 128), F32),
            pltpu.SMEM((8, 1024), jnp.int32),
            pltpu.SMEM((4, 2, 2048), F32),
            pltpu.SMEM((4, 1, 2048), F32),
            pltpu.SemaphoreType.DMA((2 * CHUNKS + 1,)),
            pltpu.SemaphoreType.DMA((5,)),
            pltpu.SemaphoreType.DMA((14,)),
            pltpu.SemaphoreType.DMA((14,)),
            pltpu.SemaphoreType.DMA((8,)),
            pltpu.SemaphoreType.DMA((4,)),
            pltpu.SemaphoreType.DMA((2,)),
            pltpu.SemaphoreType.DMA((2 * PSTEPS,)),
            pltpu.SemaphoreType.DMA((2 * PSTEPS,)),
        ],
        compiler_params=pltpu.CompilerParams(
            collective_id=0, has_side_effects=True, vmem_limit_bytes=VLIM
        ),
    )(
        coupling_left.reshape(8, RUN, INNER), inner_factor, coupling_right, iface_rows, interface_diag[None, :],
        row_scales, col_scales,
    )
    return pl.pallas_call(
        merge,
        out_shape=jax.ShapeDtypeStruct((2048, 1024), F32),
        in_specs=[any_space],
        out_specs=any_space,
        scratch_shapes=[
            pltpu.VMEM((16, 2, STRIPS, 16, 128), F32),
            pltpu.VMEM((16, RUN, 1024), F32),
            pltpu.SemaphoreType.DMA((16,)),
            pltpu.SemaphoreType.DMA((16,)),
        ],
        compiler_params=pltpu.CompilerParams(vmem_limit_bytes=63 * 2**20),
    )(strips.reshape(STRIPS, TILE_PITCH, 128))


def solution(mesh):
    in_specs = (
        P(("row", "col"), None, None),
        P(("row", "col"), None, None),
        P(("row", "col"), None, None),
        P(),
        P("row"),
        P(None, "row"),
        P(None, "col"),
    )
    out_specs = P("row", "col")
    return jax.shard_map(body, mesh=mesh, in_specs=in_specs, out_specs=out_specs, check_vma=False)
```

```python
import functools

import jax
import jax.numpy as jnp
from jax import lax
from jax.experimental import pallas as pl
from jax.experimental.pallas import tpu as pltpu
from jax.sharding import PartitionSpec as P

MESH = pl.DeviceIdType.MESH
F32 = jnp.float32
BF16 = jnp.bfloat16

VLIM = 63 * 2**20
RUN = 128
INNER = 2048
CHUNK = 256
CHUNKS = INNER // CHUNK
PIECE = 32
PITCH = 40
SRC = 128
STRIPS = 32
TILE = 512
TILE_PITCH = 512
SET = TILE // 2
PCHUNK = 8
PSTEPS = 16 // PCHUNK


def position():
    row = lax.axis_index("row")
    col = lax.axis_index("col")
    return col // 4, row // 2, col % 4, row % 2


def device(x, y, z, core):
    return (y * 2 + core, x * 4 + z)


def kernel(
    left_hbm, factor_hbm, right_hbm, iface_hbm, diag_hbm, rows_hbm, cols_hbm,
    recv2,
    right_0, right_1, right_2, right_3, right_4, right_5, right_6, right_7, right_p, factor_v, left_v, mixed_v, lpart_v, send1, recv1, tiles,
    iface_v, rows_v, diag_v, cols_v, cols8, iface_s, rows_s, diag_s,
    in_sem, small_sem, scale_send, scale_recv, send_sem1, zero_sem, recv_sem1, send_sem2, recv_sem2,
):
    x, y, z, core = position()
    zp, zb = z // 2, z % 2
    me = (y * 2 + core) * 16 + x * 4 + z
    strip = (x * 4 + y) * 2 + zb

    barrier = pltpu.get_barrier_semaphore()

    def greet(o, carry):
        pl.semaphore_signal(
            barrier, inc=1, device_id=((y * 2 + core + o // 16) % 8, (x * 4 + z + o % 16) % 16),
            device_id_type=MESH,
        )
        return carry

    own_rows = pltpu.make_async_copy(
        iface_hbm.at[pl.ds(pl.multiple_of(me // 8 * 8, 8), 8), :], iface_s, small_sem.at[0]
    )
    own_rows.start()
    right_v = [right_0, right_1, right_2, right_3, right_4, right_5, right_6, right_7]
    factor_in = []
    for c in range(CHUNKS):
        rows = pl.ds(c * CHUNK, CHUNK)
        wide = pl.ds(0, (c + 1) * CHUNK)
        for k in range(8):
            pltpu.make_async_copy(
                right_hbm.at[0, rows, pl.ds(k * RUN, RUN)], right_v[c].at[k], in_sem.at[c]
            ).start()
        factor_in.append(
            pltpu.make_async_copy(
                factor_hbm.at[0, rows, wide], factor_v.at[rows, wide], in_sem.at[CHUNKS + c]
            )
        )
        factor_in[c].start()
    left_in = pltpu.make_async_copy(left_hbm, left_v, in_sem.at[2 * CHUNKS])
    left_in.start()
    iface_in = pltpu.make_async_copy(iface_hbm, iface_v, small_sem.at[1])
    iface_in.start()
    rows_in = pltpu.make_async_copy(rows_hbm, rows_v.at[y], small_sem.at[2])
    rows_in.start()
    diag_in = pltpu.make_async_copy(diag_hbm, diag_v.at[y], small_sem.at[3])
    diag_in.start()
    cols_in = pltpu.make_async_copy(cols_hbm, cols_v.at[x * 2 + zb], small_sem.at[4])
    cols_in.start()
    lax.fori_loop(1, SRC, greet, 0)
    own_rows.wait()

    run_tile = [lax.div(iface_s[me % 8, RUN * k], 16 * RUN) for k in range(8)]

    def run_in(j):
        found = jnp.int32(0)
        for k in range(1, 8):
            found += k * (run_tile[k] == j).astype(jnp.int32)
        return found & 7

    run_of = [run_in(j) for j in range(8)]

    for c in range(CHUNKS):
        rows = pl.ds(c * CHUNK, CHUNK)
        deep = (c + 1) * CHUNK
        pltpu.make_async_copy(right_v[c], right_v[c], in_sem.at[c]).wait()
        for m in range(8):
            right_p[rows, m * RUN : (m + 1) * RUN] = right_v[c][run_of[m]]
        factor_in[c].wait()
        mixed_v[rows, :] = jnp.dot(
            factor_v[rows, :deep], right_p[:deep, :], preferred_element_type=F32
        ).astype(BF16)
    left_in.wait()

    def send_group(g, carry):
        half, to_core = g // 2, g % 2
        runs = [run_in((half * 2 + y1) * 2 + to_core) for y1 in range(2)]
        for c in range(CHUNKS):
            rows = pl.ds(c * CHUNK, CHUNK)
            deep = (c + 1) * CHUNK
            taken = jnp.concatenate([left_v[run, :, :deep] for run in runs], axis=0)
            lpart_v[:, c * CHUNK : (c + 1) * CHUNK] = lax.dot_general(
                taken, factor_v[rows, :deep], (((1,), (1,)), ((), ())), preferred_element_type=F32
            ).astype(BF16)
        for pair in range(4):
            block = jnp.dot(
                lpart_v[...], mixed_v[:, pair * 2 * RUN : (pair + 1) * 2 * RUN],
                preferred_element_type=F32,
            )
            for half_pair in range(2):
                for y1 in range(2):
                    slot = y1 * 4 + pair
                    for b in range(16):
                        base = ((b // 8) * 4 * 64 + half_pair * 32 + 4 * (b % 8)) * 16 + slot
                        send1[pl.ds((to_core * 2 + half) * (64 * 16) + base, 8, stride=8), :] = block[
                            y1 * RUN + 8 * b : y1 * RUN + 8 * b + 8,
                            half_pair * RUN : (half_pair + 1) * RUN,
                        ]

        @pl.when(g == 0)
        def _():
            pl.semaphore_wait(barrier, SRC - 1)
            rows_in.wait()
            diag_in.wait()
            cols_in.wait()
            for d in range(1, 4):
                to = device(x, (y + d) % 4, z, core)
                pltpu.make_async_remote_copy(
                    rows_v.at[y], rows_v.at[y], scale_send.at[d], scale_recv.at[d], device_id=to,
                    device_id_type=MESH,
                ).start()
                pltpu.make_async_remote_copy(
                    diag_v.at[y], diag_v.at[y], scale_send.at[3 + d], scale_recv.at[3 + d], device_id=to,
                    device_id_type=MESH,
                ).start()
            for d in range(1, 8):
                pltpu.make_async_remote_copy(
                    cols_v.at[x * 2 + zb], cols_v.at[x * 2 + zb], scale_send.at[6 + d],
                    scale_recv.at[6 + d],
                    device_id=device((x + d // 2) % 4, y, zp * 2 + (zb + d % 2) % 2, core),
                    device_id_type=MESH,
                ).start()

        send_pieces(0, to_core, half, send_sem1.at[g], zero_sem.at[half])
        return carry

    def send_pieces(part, to_core, half, sent, sent_zero):
        def piece(px, py, pz):
            index = (part * 4 + to_core * 2 + half) * 64 + (pz // 2) * 32
            index += (px * 4 + py) * 2 + pz % 2
            return (
                send1.at[pl.ds(pl.multiple_of(index * 16, 8), 16), :],
                recv1.at[pl.ds(pl.multiple_of((part * SRC + me) * PITCH + half * 16, 8), 16), :],
            )

        @pl.when(to_core == core)
        def _():
            src, dst = piece(x, y, z)
            pltpu.make_async_copy(src, dst, recv_sem1.at[part]).start()

        @pl.when(to_core != core)
        def _():
            src, dst = piece(x, y, z)
            pltpu.make_async_remote_copy(
                src, dst, sent_zero, recv_sem1.at[part],
                device_id=device(x, y, z, to_core), device_id_type=MESH,
            ).start()

        def one(o, inner):
            o = (o * 27) % 64
            px, py, pz = (x + o % 4) % 4, (y + o // 4 % 4) % 4, (z + o // 16) % 4
            src, dst = piece(px, py, pz)
            pltpu.make_async_remote_copy(
                src, dst, sent, recv_sem1.at[part],
                device_id=device(px, py, pz, to_core), device_id_type=MESH,
            ).start()
            return inner

        lax.fori_loop(1, 64, one, 0)

    lax.fori_loop(0, 4, send_group, 0)

    def send_rest(g, carry):
        send_pieces(1, g % 2, g // 2, send_sem1.at[4 + g], zero_sem.at[2 + g // 2])
        return carry

    lax.fori_loop(0, 4, send_rest, 0)

    iface_in.wait()
    run_ids = []
    for k in range(8):
        run_ids.append(lax.div(iface_v[:, k * RUN : (k + 1) * RUN].T[0:1, :], RUN))

    def placed(j):
        total = jnp.zeros((1, SRC), jnp.int32)
        for k in range(8):
            total += jnp.where(run_ids[k] // 16 == j, run_ids[k] % 16, 0)
        return total

    col_place = [placed(2 * j + zp) for j in range(4)]
    row_place = [placed(2 * j + core) for j in range(4)]
    spots = lax.broadcasted_iota(jnp.int32, (256, SRC), 0)

    def place(part):
        got = recv1.at[pl.ds(0, SRC * PIECE), :]
        pltpu.make_async_copy(got, got, recv_sem1.at[part]).wait()
        for yy in range(4):
            for xx in range(4):
                first = part * SRC * PITCH + (yy // 2) * 16 + (yy % 2) * 4 + xx
                data = jnp.concatenate(
                    [recv1[pl.ds(first + 8 * i, SRC, stride=PITCH), :] for i in range(2)], axis=1
                )
                high = data.astype(BF16)
                low = (data - high.astype(F32)).astype(BF16)
                spot = row_place[yy] * 16 + col_place[xx]
                hot = jnp.where(spots == spot, -1.0, 0.0).astype(BF16)
                tile = jnp.dot(
                    jnp.concatenate([hot, hot], axis=1), jnp.concatenate([high, low], axis=0),
                    preferred_element_type=F32,
                )
                for zz in range(2):
                    base = ((yy * 4 + xx) * 2 + zz) * TILE + part * SET
                    for p in range(16):
                        for i in range(2):
                            tiles[pl.ds(base + p * 16 + i, 8, stride=2), :] = tile[
                                p * 16 + zz * 8 : p * 16 + zz * 8 + 8, i * 128 : (i + 1) * 128
                            ]

    place(0)
    for d in range(1, 4):
        rows_v_any, diag_v_any = rows_v.at[y], diag_v.at[y]
        pltpu.make_async_remote_copy(
            rows_v_any, rows_v_any, scale_send.at[d], scale_recv.at[d],
            device_id=device(x, y, z, core), device_id_type=MESH,
        ).wait()
        pltpu.make_async_remote_copy(
            diag_v_any, diag_v_any, scale_send.at[3 + d], scale_recv.at[3 + d],
            device_id=device(x, y, z, core), device_id_type=MESH,
        ).wait()
    for d in range(1, 8):
        cols_any = cols_v.at[x * 2 + zb]
        pltpu.make_async_remote_copy(
            cols_any, cols_any, scale_send.at[6 + d], scale_recv.at[6 + d],
            device_id=device(x, y, z, core), device_id_type=MESH,
        ).wait()
    rows_to = pltpu.make_async_copy(rows_v, rows_s, small_sem.at[2])
    diag_to = pltpu.make_async_copy(diag_v, diag_s, small_sem.at[3])
    rows_to.start()
    diag_to.start()
    for xz in range(8):
        for level in range(2):
            for q in range(8):
                cols8[xz, level, q // 4, q % 4 * 2 : q % 4 * 2 + 2, :] = jnp.broadcast_to(
                    cols_v[xz, level : level + 1, q * 128 : (q + 1) * 128]
                    * (1.0 if level == 0 else 0.25),
                    (2, 128),
                )
    rows_to.wait()
    diag_to.wait()

    sub8 = lax.broadcasted_iota(jnp.int32, (8, 128), 0)
    lane8 = lax.broadcasted_iota(jnp.int32, (8, 128), 1)
    odd = sub8 % 2 == 1

    def mix_and_send(part, step):

        def mix(pp, carry):
            p = step * PCHUNK + pp
            within = 64 * part + 2 * strip
            spot = p * RUN + within
            s0 = [jnp.where(odd, rows_s[yy, 0, spot + 1], rows_s[yy, 0, spot]) for yy in range(4)]
            s1 = [jnp.where(odd, rows_s[yy, 1, spot + 1], rows_s[yy, 1, spot]) for yy in range(4)]
            diags = [
                jnp.where(odd, diag_s[yy, 0, spot + 1], diag_s[yy, 0, spot]) for yy in range(4)
            ]
            for zz in range(2):
                for h in range(2):
                    first = [cols8[xx * 2 + zz, 0, h] for xx in range(4)]
                    second = [cols8[xx * 2 + zz, 1, h] for xx in range(4)]
                    on = (sub8 // 2 + 8 * zz + 4 * h == p) & (lane8 == within + sub8 % 2)
                    on = on & (core == zp)

                    def at(yy, xx):
                        start = ((yy * 4 + xx) * 2 + zz) * TILE + part * SET + p * 16 + h * 8
                        return pl.ds(pl.multiple_of(start, 8), 8)

                    held = [[None] * 4 for _ in range(4)]
                    for xx in range(4):
                        a = [tiles[at(yy, xx), :] for yy in range(4)]
                        a[xx] = a[xx] + jnp.where(on, diags[xx], 0.0)
                        b0, b1 = (a[0] + a[1]) * s0[0], (a[0] - a[1]) * s0[1]
                        b2, b3 = (a[2] + a[3]) * s0[2], (a[2] - a[3]) * s0[3]
                        held[0][xx] = (b0 + b2) * s1[0]
                        held[2][xx] = (b0 - b2) * s1[2]
                        held[1][xx] = (b1 + b3) * s1[1]
                        held[3][xx] = (b1 - b3) * s1[3]
                    for yy in range(4):
                        a = held[yy]
                        b0, b1 = (a[0] + a[1]) * first[0], (a[0] - a[1]) * first[1]
                        b2, b3 = (a[2] + a[3]) * first[2], (a[2] - a[3]) * first[3]
                        tiles[at(yy, 0), :] = (b0 + b2) * second[0]
                        tiles[at(yy, 2), :] = (b0 - b2) * second[2]
                        tiles[at(yy, 1), :] = (b1 + b3) * second[1]
                        tiles[at(yy, 3), :] = (b1 - b3) * second[3]
            return carry

        lax.fori_loop(0, PCHUNK, mix, 0)

        chunk = part * SET + step * PCHUNK * 16

        def back(px, py, pzb):
            index = (py * 4 + px) * 2 + pzb
            return (
                tiles.at[pl.ds(pl.multiple_of(index * TILE + chunk, 8), PCHUNK * 16), :],
                recv2.at[pl.ds(pl.multiple_of(strip * TILE_PITCH + chunk, 8), PCHUNK * 16), :],
            )

        src, dst = back(x, y, zb)
        order = part * PSTEPS + step
        pltpu.make_async_copy(src, dst, recv_sem2.at[order]).start()

        def one_back(o, carry):
            o = (o * 7) % 32
            px, py, pzb = (x + o % 4) % 4, (y + o // 4 % 4) % 4, (zb + o // 16) % 2
            src, dst = back(px, py, pzb)
            pltpu.make_async_remote_copy(
                src, dst, send_sem2.at[order], recv_sem2.at[order],
                device_id=device(px, py, zp * 2 + pzb, core), device_id_type=MESH,
            ).start()
            return carry

        lax.fori_loop(1, STRIPS, one_back, 0)

    for step in range(PSTEPS):
        mix_and_send(0, step)
    place(1)
    for step in range(PSTEPS):
        mix_and_send(1, step)

    for order in range(2 * PSTEPS):
        got = recv2.at[pl.ds(0, STRIPS * PCHUNK * 16), :]
        pltpu.make_async_copy(got, got, recv_sem2.at[order]).wait()

    for g in range(8):
        sent = send1.at[pl.ds(0, 63 * 16), :]
        pltpu.make_async_copy(sent, sent, send_sem1.at[g]).wait()
    for half in range(2):
        sent = send1.at[pl.ds(0, 16), :]
        pltpu.make_async_copy(sent, sent, zero_sem.at[half]).wait()
        sent = send1.at[pl.ds(0, 16), :]
        pltpu.make_async_copy(sent, sent, zero_sem.at[2 + half]).wait()
    for order in range(2 * PSTEPS):
        sent = tiles.at[pl.ds(0, (STRIPS - 1) * PCHUNK * 16), :]
        pltpu.make_async_copy(sent, sent, send_sem2.at[order]).wait()


def merge(strips, out, got, held, in_sem, out_sem):
    sub8 = lax.broadcasted_iota(jnp.int32, (8, 128), 0)
    upper = sub8 < 4
    even = sub8 // 2 % 2 == 0

    def fetch(p, part):
        return pltpu.make_async_copy(
            strips.at[:, pl.ds(pl.multiple_of(part * SET + p * 16, 8), 16), :],
            got.at[p, part], in_sem.at[p],
        )

    def put(p):
        return pltpu.make_async_copy(
            held.at[p], out.at[pl.ds(pl.multiple_of(p * RUN, RUN), RUN), :], out_sem.at[p]
        )

    def start(p, carry):
        for part in range(2):
            fetch(p, part).start()
        return carry

    lax.fori_loop(0, 16, start, 0)

    def swap(a, b, mask, shift):
        return (
            jnp.where(mask, a, pltpu.roll(b, shift, 0)),
            jnp.where(mask, pltpu.roll(a, 8 - shift, 0), b),
        )

    def one(p, carry):
        pltpu.make_async_copy(got.at[p], got.at[p], in_sem.at[p]).wait()
        for part in range(2):
            for a in range(8):
                for h in range(2):
                    v = [got[p, part, 4 * a + k, 8 * h : 8 * h + 8, :] for k in range(4)]
                    v[0], v[2] = swap(v[0], v[2], upper, 4)
                    v[1], v[3] = swap(v[1], v[3], upper, 4)
                    v[0], v[1] = swap(v[0], v[1], even, 2)
                    v[2], v[3] = swap(v[2], v[3], even, 2)
                    for k in range(4):
                        q = 4 * h + k
                        held[
                            p, 64 * part + 8 * a : 64 * part + 8 * a + 8, q * 128 : (q + 1) * 128
                        ] = v[k]
        put(p).start()
        return carry

    lax.fori_loop(0, 16, one, 0)

    def finish(p, carry):
        put(p).wait()
        return carry

    lax.fori_loop(0, 16, finish, 0)


def body(
    coupling_left, inner_factor, coupling_right, iface_rows, interface_diag, row_scales, col_scales
):
    any_space = pl.BlockSpec(memory_space=pl.ANY)
    strips = pl.pallas_call(
        kernel,
        out_shape=jax.ShapeDtypeStruct((STRIPS * TILE_PITCH, 128), F32),
        in_specs=[any_space] * 7,
        out_specs=any_space,
        scratch_shapes=[
            *[pltpu.VMEM((8, CHUNK, RUN), BF16)] * CHUNKS,
            pltpu.VMEM((INNER, 1024), BF16),
            pltpu.VMEM((INNER, INNER), BF16),
            pltpu.VMEM((8, RUN, INNER), BF16),
            pltpu.VMEM((INNER, 1024), BF16),
            pltpu.VMEM((2 * RUN, INNER), BF16),
            pltpu.VMEM((2 * 4 * 64 * 16, 128), F32),
            pltpu.VMEM((2 * SRC * PITCH, 128), F32),
            pltpu.VMEM((STRIPS * TILE, 128), F32),
            pltpu.VMEM((SRC, 1024), jnp.int32),
            pltpu.VMEM((4, 2, 2048), F32),
            pltpu.VMEM((4, 1, 2048), F32),
            pltpu.VMEM((8, 2, 1024), F32),
            pltpu.VMEM((8, 2, 2, 8, 128), F32),
            pltpu.SMEM((8, 1024), jnp.int32),
            pltpu.SMEM((4, 2, 2048), F32),
            pltpu.SMEM((4, 1, 2048), F32),
            pltpu.SemaphoreType.DMA((2 * CHUNKS + 1,)),
            pltpu.SemaphoreType.DMA((5,)),
            pltpu.SemaphoreType.DMA((14,)),
            pltpu.SemaphoreType.DMA((14,)),
            pltpu.SemaphoreType.DMA((8,)),
            pltpu.SemaphoreType.DMA((4,)),
            pltpu.SemaphoreType.DMA((2,)),
            pltpu.SemaphoreType.DMA((2 * PSTEPS,)),
            pltpu.SemaphoreType.DMA((2 * PSTEPS,)),
        ],
        compiler_params=pltpu.CompilerParams(
            collective_id=0, has_side_effects=True, vmem_limit_bytes=VLIM
        ),
    )(
        coupling_left.reshape(8, RUN, INNER), inner_factor, coupling_right, iface_rows, interface_diag[None, :],
        row_scales, col_scales,
    )
    return pl.pallas_call(
        merge,
        out_shape=jax.ShapeDtypeStruct((2048, 1024), F32),
        in_specs=[any_space],
        out_specs=any_space,
        scratch_shapes=[
            pltpu.VMEM((16, 2, STRIPS, 16, 128), F32),
            pltpu.VMEM((16, RUN, 1024), F32),
            pltpu.SemaphoreType.DMA((16,)),
            pltpu.SemaphoreType.DMA((16,)),
        ],
        compiler_params=pltpu.CompilerParams(vmem_limit_bytes=63 * 2**20),
    )(strips.reshape(STRIPS, TILE_PITCH, 128))


def solution(mesh):
    in_specs = (
        P(("row", "col"), None, None),
        P(("row", "col"), None, None),
        P(("row", "col"), None, None),
        P(),
        P("row"),
        P(None, "row"),
        P(None, "col"),
    )
    out_specs = P("row", "col")
    return jax.shard_map(body, mesh=mesh, in_specs=in_specs, out_specs=out_specs, check_vma=False)
```
